32 devices in a mesh: dp: 1, ep: 32 (over x, y, z, core).
Axes of the slice: x: 2, y: 2, z: 4, core: 2. Of those that a mesh axis runs over, the one named last changes fastest.
Arguments:
- x: bfloat16 [1, 32, 256, 1536], P('dp', 'ep')
- expert: int32 [1, 32, 256, 2], P('dp', 'ep')
- slot: int32 [1, 32, 256, 2], P('dp', 'ep')
- gate: float32 [1, 32, 256, 2], P('dp', 'ep')
- w_gate: bfloat16 [32, 1536, 9216], P('ep')
- w_up: bfloat16 [32, 1536, 9216], P('ep')
- w_down: bfloat16 [32, 9216, 1536], P('ep')
Outputs:
- y: bfloat16 [1, 32, 256, 1536], P('dp', 'ep')
All inputs are finite; a program needn't handle non-finite values.
Results may differ from the reference program's by a relative error of at most 0.009.
Values are sent between devices in bfloat16 or wider.
A program may use at most 2 GiB of HBM per device.

```python
import jax
import jax.numpy as jnp

MEMBERS = 32
TOKENS = 256
D = 1536
FF = 9216
TOP = 2
EXPERTS = 32
SLOTS = 5 * TOKENS * TOP // (4 * EXPERTS)


def setup_inputs(seed: int = 0, part: int = 0) -> dict:
    own, k1, k2, k3, k4, k5, k6 = jax.random.split(jax.random.key(seed), 7)
    kx, ke, kl, kg = jax.random.split(jax.random.fold_in(own, part), 4)
    devices = (1, MEMBERS)
    place = jax.random.permutation(kl, jnp.arange(EXPERTS, dtype=jnp.uint32))
    slow = ((EXPERTS + (9 * place) % EXPERTS) << ((9 * place) // EXPERTS)) // EXPERTS
    wait = (jax.random.bits(ke, (*devices, TOKENS, EXPERTS), jnp.uint32) >> 10) * slow
    expert = jnp.argsort(wait, axis=-1)[..., :TOP].astype(jnp.int32)
    chosen = jax.nn.one_hot(expert, EXPERTS, dtype=jnp.int32)
    in_line = jnp.cumsum(chosen.reshape(*devices, TOKENS * TOP, EXPERTS), axis=2) - 1
    slot = jnp.sum(in_line.reshape(chosen.shape) * chosen, axis=-1)

    def one(key, rows, columns):
        return (jax.random.normal(key, (rows, columns), jnp.float32) * rows**-0.5).astype(jnp.bfloat16)

    def weights(key, rows, columns):
        return jax.lax.map(lambda k: one(k, rows, columns), jax.random.split(key, EXPERTS))

    return {
        "x": jax.random.normal(kx, (*devices, TOKENS, D), jnp.float32).astype(jnp.bfloat16),
        "expert": expert,
        "slot": slot,
        "gate": jax.nn.softmax(jax.random.normal(kg, expert.shape, jnp.float32)),
        "w_gate": weights(k1, D, FF),
        "w_up": weights(k2, D, FF),
        "w_down": weights(k3, FF, D),
    }


def einsum(form, a, b):
    return jnp.einsum(form, a.astype(jnp.float32), b.astype(jnp.float32))


def reference(x, expert, slot, gate, w_gate, w_up, w_down):
    to_expert = jax.nn.one_hot(expert, EXPERTS, dtype=jnp.bfloat16)
    to_slot = jax.nn.one_hot(slot, SLOTS, dtype=jnp.bfloat16)
    weighted = to_expert * gate[..., None].astype(jnp.bfloat16)
    dispatch = einsum("abtke,abtkc->abtec", to_expert, to_slot).astype(jnp.bfloat16)
    combine = einsum("abtke,abtkc->abtec", weighted, to_slot).astype(jnp.bfloat16)
    z = einsum("abtec,abtd->aebcd", dispatch, x).astype(jnp.bfloat16)
    h = jax.nn.silu(einsum("aebcd,edf->aebcf", z, w_gate))
    h = (h * einsum("aebcd,edf->aebcf", z, w_up)).astype(jnp.bfloat16)
    out = einsum("aebcf,efd->aebcd", h, w_down).astype(jnp.bfloat16)
    y = einsum("abtec,aebcd->abtd", combine, out)
    return y.astype(jnp.bfloat16)
```

```python
import functools

import jax
import jax.numpy as jnp
from jax import lax
from jax.experimental import pallas as pl
from jax.experimental.pallas import tpu as pltpu
from jax.sharding import PartitionSpec as P

MESH = pl.DeviceIdType.MESH
N = 32
T, D, FF = 256, 1536, 9216
C = 20
Q = D // 4
FT = 512
TILES = FF // FT
DEPTH = 4
BLOCK = 256

MASK_BITS = (0, 3, 4, 1, 2)
NEAR, FAR1, FAR2 = (0, 16, 0), (16, 8, 320), (24, 8, 480)
GROUPS = (NEAR, FAR1, FAR2)


def dot(a, b, contract=((1,), (0,))):
    return lax.dot_general(a, b, (contract, ((), ())), preferred_element_type=jnp.float32)


def partner(me, p):
    out = 0
    for b, bit in enumerate(MASK_BITS):
        mine = lax.rem(me // (1 << bit), 2)
        other = lax.rem(p // (1 << b), 2)
        out += lax.rem(mine + other, 2) * (1 << bit)
    return out


def rows_of(p):
    return pl.multiple_of(p * 16 + 64 * (p // 16) + 32 * (p // 24), 16)


def iota(shape, dim):
    return lax.broadcasted_iota(jnp.int32, shape, dim)


def kernel(x_hbm, e_hbm, s_hbm, g_hbm, wg_hbm, wu_hbm, wd_hbm, y_ref,
           x_ref, e_ref, s_ref, g_ref, zs, zse, z, zre, o, oe, r, re, acc, hn, hf, wg, wu, wd,
           in_sem, w_sem, wd_sem, dsend, drecv, rsend, rrecv):
    me = lax.axis_index("ep")
    barrier = pltpu.get_barrier_semaphore()

    @pl.loop(1, N)
    def _(p):
        pl.semaphore_signal(barrier, 1, device_id={"ep": partner(me, p)}, device_id_type=MESH)

    small = [pltpu.make_async_copy(a, b, in_sem.at[i])
             for i, (a, b) in enumerate(((e_hbm, e_ref), (s_hbm, s_ref), (g_hbm, g_ref), (x_hbm, x_ref)))]
    for c in small:
        c.start()

    def tile(t):
        slot = lax.rem(t, DEPTH)
        cols = pl.ds(pl.multiple_of(t * FT, FT), FT)
        return (pltpu.make_async_copy(wg_hbm.at[:, cols], wg.at[slot], w_sem.at[slot, 0]),
                pltpu.make_async_copy(wu_hbm.at[:, cols], wu.at[slot], w_sem.at[slot, 1]))

    def load(t):
        for c in tile(t):
            c.start()

    for t in range(DEPTH):
        load(t)
    down = pltpu.make_async_copy(wd_hbm, wd, wd_sem)
    down.start()
    for c in small:
        c.wait()

    e, s = e_ref[...], s_ref[...]
    p = jnp.zeros_like(e)
    for b, bit in enumerate(MASK_BITS):
        p += (((e >> bit) & 1) ^ ((me >> bit) & 1)) << b
    key = jnp.where(s < 16, p * 16 + s, -1)
    key4 = jnp.where((s >= 16) & (s < C), p * 4 + s - 16, -1)
    gate = g_ref[...].astype(jnp.bfloat16).astype(jnp.float32)

    row = iota((N * 16, T), 0)
    row4 = (row // 16) * 4 + lax.rem(row, 4)
    quarter = lax.rem(row // 4, 4)
    x = x_ref[...]
    hit = (row == key[0:1]) | (row == key[1:2])
    zs[...] = dot(hit.astype(jnp.bfloat16), x).astype(jnp.bfloat16)
    hit4 = (row4 == key4[0:1]) | (row4 == key4[1:2])
    part = jnp.zeros((N * 16, Q), jnp.float32)
    for q in range(4):
        part += dot((hit4 & (quarter == q)).astype(jnp.bfloat16), x[:, q * Q:(q + 1) * Q])
    zse[...] = part.astype(jnp.bfloat16)
    z[0:16, :] = zs[0:16, :]
    zre[0:16, :] = zse[0:16, :]

    pl.semaphore_wait(barrier, N - 1)

    def remote(src, dst, send, recv, p):
        return pltpu.make_async_remote_copy(
            src, dst, send, recv, device_id={"ep": partner(me, p)}, device_id_type=MESH)

    for g, (first, count, _) in enumerate(GROUPS):
        @pl.loop(max(first, 1), first + count)
        def _(p, g=g):
            b = pl.ds(pl.multiple_of(p * 16, 16), 16)
            remote(zs.at[b], z.at[pl.ds(rows_of(p), 16)], dsend.at[g, 0], drecv.at[g, 0], p).start()
            remote(zse.at[b], zre.at[b], dsend.at[g, 1], drecv.at[g, 1], p).start()

    def whole(g, packed, base, send, recv):
        first, count, rows = GROUPS[g]
        skip = 16 if first == 0 else 0
        start = rows if packed else first * 16
        b = pl.ds(start + skip, count * 16 - skip)
        return remote(base.at[b], base.at[b], send, recv, 1)

    def quarters(shape, along):
        a, b = iota(shape, along), iota(shape, 1 - along)
        same = (a // 16) * 4 + lax.rem(a, 4) == b
        return [(same & (lax.rem(a // 4, 4) == q)).astype(jnp.bfloat16) for q in range(4)]

    def arrive(g):
        first, count, rows = GROUPS[g]
        whole(g, True, z, dsend.at[g, 0], drecv.at[g, 0]).wait_recv()
        whole(g, False, zre, dsend.at[g, 1], drecv.at[g, 1]).wait_recv()
        packed = zre[first * 16:(first + count) * 16, :]
        top = rows + count * 16
        for q, pick in enumerate(quarters((count * 4, count * 16), 1)):
            z[top:top + count * 4, q * Q:(q + 1) * Q] = dot(pick, packed).astype(jnp.bfloat16)

    def gated(g, h, t):
        _, count, rows = GROUPS[g]
        slot = lax.rem(t, DEPTH)
        a = z[rows:rows + count * C, :]
        for n in range(FT // BLOCK):
            cols = slice(n * BLOCK, (n + 1) * BLOCK)
            u = dot(a, wg[slot, :, cols])
            v = dot(a, wu[slot, :, cols])
            h[:, pl.ds(pl.multiple_of(t * FT + n * BLOCK, BLOCK), BLOCK)] = (
                jax.nn.silu(u) * v).astype(jnp.bfloat16)

    def project(g, h):
        first, count, rows = GROUPS[g]

        @pl.loop(0, D // BLOCK)
        def _(n):
            cols = pl.ds(pl.multiple_of(n * BLOCK, BLOCK), BLOCK)
            o[rows:rows + count * C, cols] = dot(h[...], wd[:, cols]).astype(jnp.bfloat16)

        top = rows + count * 16
        part = jnp.zeros((count * 16, Q), jnp.float32)
        for q, pick in enumerate(quarters((count * 16, count * 4), 0)):
            part += dot(pick, o[top:top + count * 4, q * Q:(q + 1) * Q])
        oe[first * 16:(first + count) * 16, :] = part.astype(jnp.bfloat16)

        @pl.loop(max(first, 1), first + count)
        def _(p):
            b = pl.ds(pl.multiple_of(p * 16, 16), 16)
            remote(o.at[pl.ds(rows_of(p), 16)], r.at[b], rsend.at[g, 0], rrecv.at[g, 0], p).start()
            remote(oe.at[b], re.at[b], rsend.at[g, 1], rrecv.at[g, 1], p).start()

    def wait_tile(t):
        for c in tile(t):
            c.wait()

    arrive(0)

    @pl.loop(0, TILES)
    def _(t):
        wait_tile(t)
        gated(0, hn, t)

        @pl.when(t < TILES - DEPTH)
        def _():
            load(t + DEPTH)

    arrive(1)

    @pl.loop(0, TILES)
    def _(i):
        t = TILES - 1 - i

        @pl.when(i >= DEPTH)
        def _():
            wait_tile(t)

        gated(1, hf, t)

        @pl.when(t >= DEPTH)
        def _():
            load(t - DEPTH)

    down.wait()
    project(1, hf)

    arrive(2)

    @pl.loop(0, TILES)
    def _(t):
        @pl.when(t >= DEPTH)
        def _():
            wait_tile(t)

        gated(2, hf, t)

        @pl.when(t < TILES - DEPTH)
        def _():
            load(t + DEPTH)

    project(2, hf)
    project(0, hn)
    r[0:16, :] = o[0:16, :]
    re[0:16, :] = oe[0:16, :]

    for g in (1, 0, 2):
        first, count, _ = GROUPS[g]
        whole(g, False, r, rsend.at[g, 0], rrecv.at[g, 0]).wait_recv()
        whole(g, False, re, rsend.at[g, 1], rrecv.at[g, 1]).wait_recv()
        b = slice(first * 16, (first + count) * 16)
        row = first * 16 + iota((count * 16, T), 0)
        row4 = (row // 16) * 4 + lax.rem(row, 4)
        quarter = lax.rem(row // 4, 4)
        w = jnp.where(row == key[0:1], gate[0:1], 0.0) + jnp.where(row == key[1:2], gate[1:2], 0.0)
        w4 = jnp.where(row4 == key4[0:1], gate[0:1], 0.0) + jnp.where(row4 == key4[1:2], gate[1:2], 0.0)
        w = w.astype(jnp.bfloat16)
        for q in range(4):
            cols = slice(q * Q, (q + 1) * Q)
            mine = jnp.where(quarter == q, w4, 0.0).astype(jnp.bfloat16)
            total = dot(w, r[b, cols], ((0,), (0,))) + dot(mine, re[b, :], ((0,), (0,)))
            if g == 1:
                acc[:, cols] = total
            elif g == 0:
                acc[:, cols] += total
            else:
                y_ref[:, cols] = (acc[:, cols] + total).astype(jnp.bfloat16)

    for g in range(3):
        whole(g, False, zs, dsend.at[g, 0], drecv.at[g, 0]).wait_send()
        whole(g, False, zse, dsend.at[g, 1], drecv.at[g, 1]).wait_send()
        whole(g, True, o, rsend.at[g, 0], rrecv.at[g, 0]).wait_send()
        whole(g, False, oe, rsend.at[g, 1], rrecv.at[g, 1]).wait_send()


def solution(mesh):
    def step(x, expert, slot, gate, w_gate, w_up, w_down):
        bf16 = jnp.bfloat16
        flat = lambda v: v.reshape(T, 2).T
        any_ = pl.BlockSpec(memory_space=pl.ANY)
        vmem = pltpu.VMEM
        y = pl.pallas_call(
            kernel,
            out_shape=jax.ShapeDtypeStruct((T, D), bf16),
            in_specs=[any_] * 7,
            out_specs=pl.BlockSpec(memory_space=pltpu.VMEM),
            scratch_shapes=[
                vmem((T, D), bf16),
                vmem((2, T), jnp.int32),
                vmem((2, T), jnp.int32),
                vmem((2, T), jnp.float32),
                vmem((N * 16, D), bf16),
                vmem((N * 16, Q), bf16),
                vmem((N * C, D), bf16),
                vmem((N * 16, Q), bf16),
                vmem((N * C, D), bf16),
                vmem((N * 16, Q), bf16),
                vmem((N * 16, D), bf16),
                vmem((N * 16, Q), bf16),
                vmem((T, D), jnp.float32),
                vmem((16 * C, FF), bf16),
                vmem((8 * C, FF), bf16),
                vmem((DEPTH, D, FT), bf16),
                vmem((DEPTH, D, FT), bf16),
                vmem((FF, D), bf16),
                pltpu.SemaphoreType.DMA((4,)),
                pltpu.SemaphoreType.DMA((DEPTH, 2)),
                pltpu.SemaphoreType.DMA,
                pltpu.SemaphoreType.DMA((3, 2)),
                pltpu.SemaphoreType.DMA((3, 2)),
                pltpu.SemaphoreType.DMA((3, 2)),
                pltpu.SemaphoreType.DMA((3, 2)),
            ],
            compiler_params=pltpu.CompilerParams(
                collective_id=0, has_side_effects=True, vmem_limit_bytes=67043328
            ),
            name="moe",
        )(x.reshape(T, D), flat(expert), flat(slot), flat(gate), w_gate[0], w_up[0], w_down[0])
        return y.reshape(1, 1, T, D)

    row = P("dp", "ep", None, None)
    weight = P("ep", None, None)
    return jax.shard_map(
        step, mesh=mesh, in_specs=(row,) * 4 + (weight,) * 3, out_specs=row, check_vma=False
    )
```
